32 devices in a mesh: ma: 4 (over x, core), ell: 8 (over z, y).
Axes of the slice: x: 2, y: 2, z: 4, core: 2. Of those that a mesh axis runs over, the one named last changes fastest.
Arguments:
- legendre: bfloat16 [3, 2048, 2, 4096], P(None, 'ma', None, 'ell'), may hold values from -6 to 6
- harmonics: bfloat16 [2048, 3, 2, 4, 4096], P('ma', None, None, None, 'ell'), may hold values from -0.0014648438 to 0.0014648438
- slot_orders: int32 [2048], replicated, may hold values from 0 to 2047, each once
- cycle_index: int32 [2], replicated, may hold values from 2048 to 4095
Outputs:
- maps: float32 [4, 3, 4, 8192], P('ma', None, None, 'ell')
The draws below stay inside these ranges and needn't reach their ends.
Inputs may be any that keep to these rules, and one draw needn't show every extreme that they name: `slot_orders`: every number from 0 to 2047 appears once.
All inputs are finite; a program needn't handle non-finite values.
Results may differ from the reference program's by a relative error of at most 0.0003.
Values sent between devices are 32-bit elements; how exact they have to be, the bound alone decides.
A program may use at most 128 MiB of HBM per device.

```python
import math
import jax
import jax.numpy as jnp
from jax import lax

L = 4096
COMPS = 4
SLOTS = 2048
NPIX = 8192
RPAIRS = 2


def steps_of(rng, extent, pieces, low, largest):
    factor_of, own = 1.0, jax.random.fold_in(rng, 6)
    for axis_at, parts in pieces:
        heights = jnp.exp(jax.random.uniform(jax.random.fold_in(own, axis_at), (parts,), jnp.float32, low / len(pieces), largest / len(pieces)))
        factor_of = factor_of * jnp.repeat(heights, extent[axis_at] // parts).reshape([-1 if axis == axis_at else 1 for axis in range(len(extent))])
    return factor_of


def gaussian(own_key, shape, width, most, pieces=(), held_as=jnp.bfloat16):
    factor_of = steps_of(own_key, shape, pieces, -0.22, 0.18) if pieces else 1.0
    result = jax.random.normal(own_key, shape, jnp.float32) * width * factor_of
    return jnp.minimum(jnp.maximum(result, -most), most).astype(held_as)


def setup_inputs(seed: int = 0) -> dict:
    splits = jax.random.split(jax.random.key(seed), 5)
    legendre = gaussian(splits[0], (3, SLOTS, RPAIRS, L), 1.0, 6.0, ((1, 4), (3, 8)))
    harmonics = gaussian(splits[1], (SLOTS, 3, 2, COMPS, L), (L * L) ** -0.5, 0.0014648438, ((0, 4), (4, 8)))
    slot_orders = jax.random.permutation(splits[2], SLOTS).astype(jnp.int32)
    cycle_index = jax.random.randint(splits[3], (RPAIRS,), L // 2, L).astype(jnp.int32)
    return dict(legendre=legendre, harmonics=harmonics, slot_orders=slot_orders, cycle_index=cycle_index)


def column_weights(lower_order, first_column, columns_count, full_width):
    columns = first_column + jnp.arange(columns_count, dtype=jnp.int32)
    boundary = (full_width - 1 - lower_order)[:, None]
    lower_part = (columns[None, :] < boundary).astype(jnp.float32)
    upper_part = ((columns[None, :] >= boundary) & (columns[None, :] < full_width - 1)).astype(jnp.float32)
    lower_sign = (1 - 2 * (columns[None, :] % 2)).astype(jnp.float32)
    upper_sign = (1 - 2 * ((columns[None, :] + 1 + lower_order[:, None]) % 2)).astype(jnp.float32)
    return jnp.stack([lower_part, lower_part * lower_sign, upper_part, upper_part * upper_sign], axis=1)


def spin_fields(plain, plus, minus):
    hemisphere = jnp.array([1.0, -1.0], jnp.float32).reshape(1, 1, 1, 2, 1, 1, 1)
    minus = minus * hemisphere
    temp_real = plain[:, :, :, :, 0]
    temp_imag = plain[:, :, :, :, 1]
    eplus_real = plus[:, :, :, :, 0, 0]
    eplus_imag = plus[:, :, :, :, 0, 1]
    bplus_real = plus[:, :, :, :, 1, 0]
    bplus_imag = plus[:, :, :, :, 1, 1]
    eminus_real = minus[:, :, :, :, 0, 0]
    eminus_imag = minus[:, :, :, :, 0, 1]
    bminus_real = minus[:, :, :, :, 1, 0]
    bminus_imag = minus[:, :, :, :, 1, 1]
    stokes_q_real = -(eplus_real - bminus_imag)
    stokes_q_imag = -(eplus_imag + bminus_real)
    stokes_u_real = -(bplus_real + eminus_imag)
    stokes_u_imag = -(bplus_imag - eminus_real)
    return jnp.stack([jnp.stack([temp_real, temp_imag]), jnp.stack([stokes_q_real, stokes_q_imag]), jnp.stack([stokes_u_real, stokes_u_imag])])


def reference(legendre, harmonics, slot_orders, cycle_index):
    highest = lax.Precision.HIGHEST
    block = min(16, SLOTS)

    def one_block(index):
        start = index * block
        tables = lax.dynamic_slice_in_dim(legendre, start, block, 1).astype(jnp.float32)
        coeffs = lax.dynamic_slice_in_dim(harmonics, start, block, 0).astype(jnp.float32)
        lower_order = lax.dynamic_slice_in_dim(slot_orders, start, block, 0)
        weights = column_weights(lower_order, 0, L, L)
        packed = coeffs[:, None] * weights[:, :, None, None, None, :]
        plain = jnp.einsum('srj,sqpcj->srqpc', tables[0], packed[:, :, 0], precision=highest)
        plus = jnp.einsum('srj,sqkpcj->srqkpc', tables[1], packed[:, :, 1:3], precision=highest)
        minus = jnp.einsum('srj,sqkpcj->srqkpc', tables[2], packed[:, :, 1:3], precision=highest)
        plain = plain.reshape(block, RPAIRS, 2, 2, 2, COMPS)
        plus = plus.reshape(block, RPAIRS, 2, 2, 2, 2, COMPS)
        minus = minus.reshape(block, RPAIRS, 2, 2, 2, 2, COMPS)
        return spin_fields(plain, plus, minus)

    blocks = lax.map(one_block, jnp.arange(SLOTS // block, dtype=jnp.int32))
    cycle_sums = blocks.transpose(6, 4, 1, 2, 7, 5, 0, 3).reshape(2 * RPAIRS, 3, 2, COMPS, 2, SLOTS)
    lower_all = slot_orders
    upper_all = L - 1 - lower_all
    coeff = jnp.zeros((2 * RPAIRS, 3, 2, COMPS, L), jnp.float32)
    coeff = coeff.at[..., lower_all].set(cycle_sums[..., 0, :]).at[..., upper_all].set(cycle_sums[..., 1, :])
    shift = jnp.concatenate([cycle_index, cycle_index]) % 2
    orders = jnp.arange(L, dtype=jnp.int32)
    phase = ((orders[None, :] * shift[:, None]) % (2 * NPIX)).astype(jnp.float32) * (math.pi / NPIX)
    factor = jnp.where(orders == 0, 1.0, 2.0).astype(jnp.float32)
    cosine = (jnp.cos(phase) * factor)[:, None, None, :]
    sine = (jnp.sin(phase) * factor)[:, None, None, :]
    real_part = coeff[:, :, 0]
    imag_part = coeff[:, :, 1]
    shifted_real = real_part * cosine - imag_part * sine
    shifted_imag = real_part * sine + imag_part * cosine
    spectrum = shifted_real + 1j * shifted_imag
    padded = jnp.pad(spectrum, ((0, 0), (0, 0), (0, 0), (0, NPIX - L)))
    maps = jnp.real(jnp.fft.ifft(padded, axis=-1)) * NPIX
    return maps.astype(jnp.float32)
```

```python
import functools
import math

import jax
import jax.numpy as jnp
import numpy as np
from jax import lax
from jax.experimental import pallas as pl
from jax.experimental.pallas import tpu as pltpu
from jax.sharding import PartitionSpec as P


def column_weights(lower_order, first_column, columns_count, full_width):
    columns = first_column + jnp.arange(columns_count, dtype=jnp.int32)
    boundary = (full_width - 1 - lower_order)[:, None]
    lower_part = (columns[None, :] < boundary).astype(jnp.float32)
    upper_part = ((columns[None, :] >= boundary) & (columns[None, :] < full_width - 1)).astype(
        jnp.float32
    )
    lower_sign = (1 - 2 * (columns[None, :] % 2)).astype(jnp.float32)
    upper_sign = (1 - 2 * ((columns[None, :] + 1 + lower_order[:, None]) % 2)).astype(jnp.float32)
    return jnp.stack(
        [lower_part, lower_part * lower_sign, upper_part, upper_part * upper_sign], axis=1
    )


def spin_fields(plain, plus, minus):
    hemisphere = jnp.array([1.0, -1.0], jnp.float32).reshape(1, 1, 1, 2, 1, 1, 1)
    minus = minus * hemisphere
    temp_real = plain[:, :, :, :, 0]
    temp_imag = plain[:, :, :, :, 1]
    eplus_real = plus[:, :, :, :, 0, 0]
    eplus_imag = plus[:, :, :, :, 0, 1]
    bplus_real = plus[:, :, :, :, 1, 0]
    bplus_imag = plus[:, :, :, :, 1, 1]
    eminus_real = minus[:, :, :, :, 0, 0]
    eminus_imag = minus[:, :, :, :, 0, 1]
    bminus_real = minus[:, :, :, :, 1, 0]
    bminus_imag = minus[:, :, :, :, 1, 1]
    stokes_q_real = -(eplus_real - bminus_imag)
    stokes_q_imag = -(eplus_imag + bminus_real)
    stokes_u_real = -(bplus_real + eminus_imag)
    stokes_u_imag = -(bplus_imag - eminus_real)
    return jnp.stack(
        [
            jnp.stack([temp_real, temp_imag]),
            jnp.stack([stokes_q_real, stokes_q_imag]),
            jnp.stack([stokes_u_real, stokes_u_imag]),
        ]
    )


def place_orders(cycle_orders, lower_all):
    highest = lax.Precision.HIGHEST
    half = lower_all.shape[0]
    width = min(512, half)
    pieces = []
    for start in range(0, half, width):
        targets = start + jnp.arange(width, dtype=jnp.int32)
        onehot = (lower_all[:, None] == targets[None, :]).astype(jnp.float32)
        pieces.append(jnp.einsum("abcdes,sm->abcdem", cycle_orders, onehot, precision=highest))
    placed = jnp.concatenate(pieces, axis=-1)
    return jnp.concatenate([placed[..., 0, :], jnp.flip(placed[..., 1, :], axis=-1)], axis=-1)


def cycle_synthesis(coeff, shift, first_group, group_count):
    highest = lax.Precision.HIGHEST
    cycles_count = coeff.shape[0]
    components = coeff.shape[3]
    orders_count = coeff.shape[-1]
    pixels = 2 * orders_count
    outer = pixels // 128
    groups = orders_count // 128
    orders = jnp.arange(orders_count, dtype=jnp.int32)
    phase = (orders[None, :] * shift[:, None] % (2 * pixels)).astype(jnp.float32) * (
        math.pi / pixels
    )
    factor = jnp.where(orders == 0, 1.0, 2.0).astype(jnp.float32)
    cosine = (jnp.cos(phase) * factor)[:, None, None, :]
    sine = (jnp.sin(phase) * factor)[:, None, None, :]
    real_part = coeff[:, :, 0]
    imag_part = coeff[:, :, 1]
    shifted_real = (real_part * cosine - imag_part * sine).reshape(
        cycles_count, 3, components, groups, 128
    )
    shifted_imag = (real_part * sine + imag_part * cosine).reshape(
        cycles_count, 3, components, groups, 128
    )
    group_ids = jnp.arange(groups, dtype=jnp.int32)
    outer_ids = jnp.arange(outer, dtype=jnp.int32)
    inner_ids = jnp.arange(128, dtype=jnp.int32)
    angle_one = (group_ids[:, None] * outer_ids[None, :] % outer).astype(jnp.float32) * (
        2.0 * math.pi / outer
    )
    cos_one = jnp.cos(angle_one)
    sin_one = jnp.sin(angle_one)
    first_real = jnp.einsum(
        "xyzab,ak->xyzkb", shifted_real, cos_one, precision=highest
    ) - jnp.einsum("xyzab,ak->xyzkb", shifted_imag, sin_one, precision=highest)
    first_imag = jnp.einsum(
        "xyzab,ak->xyzkb", shifted_real, sin_one, precision=highest
    ) + jnp.einsum("xyzab,ak->xyzkb", shifted_imag, cos_one, precision=highest)
    angle_two = (outer_ids[:, None] * inner_ids[None, :] % pixels).astype(jnp.float32) * (
        2.0 * math.pi / pixels
    )
    cos_two = jnp.cos(angle_two)
    sin_two = jnp.sin(angle_two)
    twist_real = first_real * cos_two - first_imag * sin_two
    twist_imag = first_real * sin_two + first_imag * cos_two
    local_ids = first_group + jnp.arange(group_count, dtype=jnp.int32)
    angle_three = (inner_ids[:, None] * local_ids[None, :] % 128).astype(jnp.float32) * (
        2.0 * math.pi / 128
    )
    cos_three = jnp.cos(angle_three)
    sin_three = jnp.sin(angle_three)
    result = jnp.einsum("xyzkb,bq->xyzqk", twist_real, cos_three, precision=highest) - jnp.einsum(
        "xyzkb,bq->xyzqk", twist_imag, sin_three, precision=highest
    )
    return result.reshape(cycles_count, 3, components, group_count * outer)


def general_body(legendre, harmonics, slot_orders, cycle_index):
    ell_count = lax.axis_size("ell")
    slots_here = harmonics.shape[0]
    columns_here = harmonics.shape[-1]
    components = harmonics.shape[3]
    full_width = 2 * slot_orders.shape[0]
    pairs = cycle_index.shape[0]
    lower_here = lax.dynamic_slice_in_dim(
        slot_orders, lax.axis_index("ma") * slots_here, slots_here
    )
    weights = column_weights(
        lower_here, lax.axis_index("ell") * columns_here, columns_here, full_width
    ).astype(jnp.bfloat16)
    packed = harmonics[:, None] * weights[:, :, None, None, None, :]
    plain = jnp.einsum(
        "srj,sqpcj->srqpc", legendre[0], packed[:, :, 0], preferred_element_type=jnp.float32
    )
    plus = jnp.einsum(
        "srj,sqkpcj->srqkpc", legendre[1], packed[:, :, 1:3], preferred_element_type=jnp.float32
    )
    minus = jnp.einsum(
        "srj,sqkpcj->srqkpc", legendre[2], packed[:, :, 1:3], preferred_element_type=jnp.float32
    )
    plain = plain.reshape(slots_here, pairs, 2, 2, 2, components)
    plus = plus.reshape(slots_here, pairs, 2, 2, 2, 2, components)
    minus = minus.reshape(slots_here, pairs, 2, 2, 2, 2, components)
    fields = spin_fields(plain, plus, minus)
    cycle_sums = fields.transpose(5, 3, 0, 1, 6, 4, 2).reshape(
        2 * pairs, 3, 2, components, 2, slots_here
    )
    summed = lax.psum(cycle_sums, "ell")
    cycle_orders = lax.all_to_all(summed, "ma", split_axis=0, concat_axis=5, tiled=True)
    slot_ids = jnp.arange(slot_orders.shape[0], dtype=jnp.int32)
    lower_all = slot_orders[slot_ids]
    coeff = place_orders(cycle_orders, lower_all)
    cycles_here = cycle_orders.shape[0]
    cycle_ids = lax.axis_index("ma") * cycles_here + jnp.arange(cycles_here, dtype=jnp.int32)
    shift = cycle_index[cycle_ids % pairs] % 2
    per_device = 128 // ell_count
    return cycle_synthesis(coeff, shift, lax.axis_index("ell") * per_device, per_device)


LANES = 128
NT = (((1,), (1,)), ((), ()))


def rotate_sums(group, lane_tile, sub_pair):
    turned = None
    for step in range(4):
        mixed = group[step]
        for tile in range(1, 4):
            mixed = jnp.where(sub_pair == tile, group[(tile + step) % 4], mixed)
        if step == 0:
            turned = mixed
        else:
            mixed = pltpu.roll(mixed, 2 * step, 0)
            turned = jnp.where((sub_pair - lane_tile) % 4 == step, mixed, turned)
    return turned


def sums_kernel(full_width, start_ref, orders_ref, table_ref, packed_ref, out_ref, weight_ref, part_ref):
    step = pl.program_id(0)
    slots = orders_ref.shape[0]
    quads = slots // 4
    all_quads = pl.num_programs(0) * quads
    rows = slots * 8
    lower = jnp.broadcast_to(orders_ref[...][:, None, :], (slots, 8, LANES)).reshape(rows, LANES)
    row = lax.broadcasted_iota(jnp.int32, (rows, LANES), 0)
    lane = lax.broadcasted_iota(jnp.int32, (rows, LANES), 1)
    column = start_ref[0] + ((row % 8) // 2) * LANES + lane
    is_lower = column < full_width - 1 - lower
    is_upper = jnp.logical_and(jnp.logical_not(is_lower), column < full_width - 1)
    lower_sign = (1 - 2 * (column % 2)).astype(jnp.float32)
    upper_sign = (1 - 2 * ((column + 1 + lower) % 2)).astype(jnp.float32)
    lower_part = jnp.where(is_lower, 1.0, 0.0)
    upper_part = jnp.where(is_upper, 1.0, 0.0)
    weight_ref[0] = lower_part.astype(jnp.bfloat16)
    weight_ref[1] = (lower_part * lower_sign).astype(jnp.bfloat16)
    weight_ref[2] = upper_part.astype(jnp.bfloat16)
    weight_ref[3] = (upper_part * upper_sign).astype(jnp.bfloat16)

    sub_pair = lax.broadcasted_iota(jnp.int32, (8, LANES), 0) // 2
    lane8 = lax.broadcasted_iota(jnp.int32, (8, LANES), 1)
    lane_tile = (lane8 % 16) // 4

    def one_quad(quad, carry):
        base = pl.multiple_of(quad * 32, 32)
        weights = [weight_ref[q, pl.ds(base, 32), :] for q in range(4)]
        tables = [table_ref[t, pl.ds(base, 32), :] for t in range(3)]
        first = pl.multiple_of(quad * 384, 32)
        where_to = pl.multiple_of((step * quads + quad) * 8, 8)
        left = jnp.concatenate([tables[0] * w for w in weights], axis=0)
        right = jnp.concatenate(
            [packed_ref[pl.ds(first + 96 * g, 32), :] for g in range(4)], axis=0
        )
        product = lax.dot_general(left, right, NT, preferred_element_type=jnp.float32)
        group = []
        for q in range(4):
            chosen = product[q * 32 : q * 32 + 8]
            for g in range(1, 4):
                chosen = jnp.where(
                    lane8 // 32 == g, product[q * 32 + g * 8 : q * 32 + g * 8 + 8], chosen
                )
            group.append(chosen)
        part_ref[0, pl.ds(where_to, 8), :] = rotate_sums(group, lane_tile, sub_pair)
        for p in range(2):
            left = jnp.concatenate(
                [
                    tables[t][p * 16 : p * 16 + 16] * w[p * 16 : p * 16 + 16]
                    for t in (1, 2)
                    for w in weights
                ],
                axis=0,
            )
            right = jnp.concatenate(
                [packed_ref[pl.ds(first + 96 * (2 * p + g) + 32, 64), :] for g in range(2)], axis=0
            )
            product = lax.dot_general(left, right, NT, preferred_element_type=jnp.float32)
            for t in range(2):
                group = []
                for q in range(4):
                    at = (t * 4 + q) * 16
                    group.append(
                        jnp.where(lane8 < 64, product[at : at + 8], product[at + 8 : at + 16])
                    )
                part_ref[1 + 2 * p + t, pl.ds(where_to, 8), :] = rotate_sums(
                    group, lane_tile, sub_pair
                )
        return carry

    lax.fori_loop(0, quads, one_quad, 0, unroll=UNROLL)

    @pl.when(step == pl.num_programs(0) - 1)
    def _():
        sub = lax.broadcasted_iota(jnp.int32, (8, LANES), 0)
        low = sub < 4
        turn_sign = jnp.where(low, -1.0, 1.0)

        def kind_tile(turned, at):
            real = turned[at : at + 8] + turned[at + 8 : at + 16]
            imag = turned[at + 16 : at + 24] + turned[at + 24 : at + 32]
            real = real + pltpu.roll(real, 4, 0)
            imag = imag + pltpu.roll(imag, 4, 0)
            return jnp.where(low, real, imag)

        for h in range(2):
            for south in range(2):
                for r in range(2):
                    qr = (h * 2 + south) * 2 + r
                    cycle = south * 2 + r
                    row0 = cycle * 24 * 8 + h * 4
                    turned = [
                        part_ref[i, pl.ds(qr, all_quads_static(part_ref), stride=8), :].T
                        for i in range(5)
                    ]
                    for g in range(4):
                        at = 64 * (g % 2)
                        plus = turned[1 + 2 * (g // 2)]
                        minus = turned[2 + 2 * (g // 2)]
                        temp = kind_tile(turned[0], g * 32)
                        e_plus = kind_tile(plus, at)
                        b_plus = kind_tile(plus, at + 32)
                        e_minus = kind_tile(minus, at)
                        b_minus = kind_tile(minus, at + 32)
                        hemisphere = turn_sign * (-1.0 if south else 1.0)
                        e_turn = pltpu.roll(e_minus, 4, 0) * hemisphere
                        b_turn = pltpu.roll(b_minus, 4, 0) * hemisphere
                        fields = (temp, -(e_plus + b_turn), e_turn - b_plus)
                        for f in range(3):
                            out_ref[pl.ds(row0 + f * 64 + g, 8, stride=8), :] = fields[f]


def all_quads_static(part_ref):
    return part_ref.shape[1] // 8


UNROLL = 2


def table_sums(legendre, harmonics, lower_here, first_column, full_width, interpret=False):
    slots = harmonics.shape[0]
    tables = (
        legendre.reshape(3, slots, 2, 4, LANES).transpose(0, 1, 3, 2, 4).reshape(3, slots * 8, LANES)
    )
    packed = (
        harmonics.reshape(slots, 3, 2, 4, 4, LANES)
        .transpose(0, 1, 2, 4, 3, 5)
        .reshape(slots * 96, LANES)
    )
    orders = jnp.broadcast_to(lower_here[:, None], (slots, LANES))
    block = 32
    return pl.pallas_call(
        functools.partial(sums_kernel, full_width),
        grid=(slots // block,),
        in_specs=[
            pl.BlockSpec(memory_space=pltpu.SMEM),
            pl.BlockSpec((block, LANES), lambda i: (i, 0)),
            pl.BlockSpec((3, block * 8, LANES), lambda i: (0, i, 0)),
            pl.BlockSpec((block * 96, LANES), lambda i: (i, 0)),
        ],
        out_specs=pl.BlockSpec((768, LANES), lambda i: (0, 0)),
        out_shape=jax.ShapeDtypeStruct((768, LANES), jnp.float32),
        scratch_shapes=[
            pltpu.VMEM((4, block * 8, LANES), jnp.bfloat16),
            pltpu.VMEM((5, slots * 2, LANES), jnp.float32),
        ],
        compiler_params=pltpu.CompilerParams(
            dimension_semantics=("arbitrary",), vmem_limit_bytes=64_000_000
        ),
        interpret=interpret,
    )(first_column.reshape(1), orders, tables, packed)


def synthesis_kernel(
    sources, scalars_ref, orders_ref, sums_ref, phase_ref, first_ref, twist_ref, last_ref,
    out_ref, left_ref, right_ref
):
    highest = lax.Precision.HIGHEST
    owners = sums_ref.shape[0] // sources
    tall = left_ref.shape[0] // 9
    tall_ids = lax.broadcasted_iota(jnp.int32, (tall, LANES), 0)
    lane_rows = lax.broadcasted_iota(jnp.int32, (LANES, LANES), 0)
    for owner in range(owners):
        total = sums_ref[owner * sources]
        for source in range(1, sources):
            total = total + sums_ref[owner * sources + source]
        high = total.astype(jnp.bfloat16).astype(jnp.float32)
        rest = total - high
        middle = rest.astype(jnp.bfloat16).astype(jnp.float32)
        pieces = (high, middle, rest - middle)
        for k in range(8):
            j = owner * 8 + k
            order = orders_ref[j : j + 1, :]
            right_ref[:, j * LANES : (j + 1) * LANES] = jnp.where(
                lane_rows == order % LANES, 1.0, 0.0
            ).astype(jnp.bfloat16)
            here = tall_ids == order // LANES
            for rr in range(3):
                for i in range(3):
                    at = (rr * 3 + i) * tall
                    piece = pieces[i][rr * 8 + k : rr * 8 + k + 1, :]
                    left_ref[at : at + tall, j * LANES : (j + 1) * LANES] = jnp.where(
                        here, piece, 0.0
                    ).astype(jnp.bfloat16)
    placed = lax.dot_general(
        left_ref[...], right_ref[...], NT, preferred_element_type=jnp.float32
    )
    shifted = scalars_ref[0] == 1
    factor = phase_ref[2]
    cosine = jnp.where(shifted, phase_ref[0], factor)
    sine = jnp.where(shifted, phase_ref[1], 0.0)
    half = 2 * tall
    for rr in range(3):
        at = rr * 3 * tall
        value = (
            placed[at : at + tall]
            + placed[at + tall : at + 2 * tall]
            + placed[at + 2 * tall : at + 3 * tall]
        )
        is_real = scalars_ref[1 + rr] == 0
        spectrum = jnp.concatenate(
            [
                value * jnp.where(is_real, cosine, -sine),
                value * jnp.where(is_real, sine, cosine),
            ],
            axis=0,
        )
        first = jnp.dot(
            first_ref[...], spectrum, precision=highest, preferred_element_type=jnp.float32
        )
        real, imag = first[:half], first[half:]
        twisted = jnp.concatenate(
            [
                real * twist_ref[0] - imag * twist_ref[1],
                real * twist_ref[1] + imag * twist_ref[0],
            ],
            axis=1,
        )
        both = lax.dot_general(
            last_ref[...], twisted, NT, precision=highest, preferred_element_type=jnp.float32
        )
        pixels = jnp.concatenate([both[:64], both[64:]], axis=1)
        for e in range(out_ref.shape[0]):
            out_ref[e, rr * 8 : rr * 8 + 8, :] = pixels[e * 8 : e * 8 + 8]


def synthesis_tables(orders_count):
    pixels = 2 * orders_count
    tall = orders_count // LANES
    half = 2 * tall
    orders = np.arange(orders_count).reshape(tall, LANES)
    factor = np.where(orders == 0, 1.0, 2.0)
    angle = orders * (np.pi / pixels)
    phase = np.stack([np.cos(angle) * factor, np.sin(angle) * factor, factor])
    angle = (np.arange(half)[:, None] * np.arange(tall)[None, :] % half) * (2 * np.pi / half)
    first = np.block([[np.cos(angle), -np.sin(angle)], [np.sin(angle), np.cos(angle)]])
    angle = np.arange(half)[:, None] * np.arange(LANES)[None, :] * (2 * np.pi / pixels)
    twist = np.stack([np.cos(angle), np.sin(angle)])
    ids = np.concatenate([np.arange(0, LANES, 2), np.arange(1, LANES, 2)])
    angle = (ids[:, None] * np.arange(LANES)[None, :] % LANES) * (2 * np.pi / LANES)
    last = np.concatenate([np.cos(angle), -np.sin(angle)], axis=1)
    return [jnp.asarray(t, jnp.float32) for t in (phase, first, twist, last)]


def synthesis(received, orders, scalars, sources, orders_count, interpret=False):
    tall = orders_count // LANES
    vmem = pl.BlockSpec(memory_space=pltpu.VMEM)
    return pl.pallas_call(
        functools.partial(synthesis_kernel, sources),
        in_specs=[pl.BlockSpec(memory_space=pltpu.SMEM)] + [vmem] * 6,
        out_specs=vmem,
        out_shape=jax.ShapeDtypeStruct((sources, 24, LANES), jnp.float32),
        scratch_shapes=[
            pltpu.VMEM((9 * tall, orders_count), jnp.bfloat16),
            pltpu.VMEM((LANES, orders_count), jnp.bfloat16),
        ],
        compiler_params=pltpu.CompilerParams(vmem_limit_bytes=32 * 1024 * 1024),
        interpret=interpret,
    )(scalars, orders, received, *synthesis_tables(orders_count))


def slot_layout(slot_orders, owners):
    full_width = 2 * slot_orders.shape[0]
    lower = slot_orders.reshape(owners, LANES, 4).transpose(0, 2, 1)
    return jnp.stack([lower, full_width - 1 - lower], axis=1).reshape(owners * 8, LANES)


def packed_body(legendre, harmonics, slot_orders, cycle_index):
    owners = lax.axis_size("ma")
    sources = lax.axis_size("ell")
    slots_here = harmonics.shape[0]
    columns_here = harmonics.shape[-1]
    full_width = 2 * slot_orders.shape[0]
    pairs = cycle_index.shape[0]
    me, part = lax.axis_index("ma"), lax.axis_index("ell")
    lower_here = lax.dynamic_slice_in_dim(slot_orders, me * slots_here, slots_here)
    sums = table_sums(legendre, harmonics, lower_here, part * columns_here, full_width)
    received = lax.all_to_all(
        sums.reshape(owners * sources, 24, LANES), ("ma", "ell"), 0, 0, tiled=True
    )
    shift = cycle_index[me % pairs] % 2
    row = part * 3 + jnp.arange(3, dtype=jnp.int32)
    scalars = jnp.concatenate([shift[None], (row // 4) % 2])
    maps = synthesis(received, slot_layout(slot_orders, owners), scalars, sources, full_width)
    pixels = lax.all_to_all(maps, "ell", 0, 0, tiled=True)
    fields = pixels.reshape(3, 2, 4, 8, LANES)
    return (fields[:, 0] + fields[:, 1]).reshape(1, 3, 4, 8 * LANES)


def body(legendre, harmonics, slot_orders, cycle_index):
    owners, sources = lax.axis_size("ma"), lax.axis_size("ell")
    slots, kinds, parts, components, columns = harmonics.shape
    pairs = cycle_index.shape[0]
    fits = (
        (pairs, components, columns, slots) == (2, 4, 4 * LANES, 4 * LANES)
        and owners == 2 * pairs
        and kinds * parts * components == 3 * sources
        and slot_orders.shape[0] * 4 == sources * 8 * LANES
    )
    chosen = packed_body if fits else general_body
    return chosen(legendre, harmonics, slot_orders, cycle_index)


def solution(mesh):
    return jax.shard_map(
        body,
        mesh=mesh,
        in_specs=(P(None, "ma", None, "ell"), P("ma", None, None, None, "ell"), P(), P()),
        out_specs=P("ma", None, None, "ell"),
        check_vma=False,
    )
```

```python
import functools
import math

import jax
import jax.numpy as jnp
import numpy as np
from jax import lax
from jax.experimental import pallas as pl
from jax.experimental.pallas import tpu as pltpu
from jax.sharding import PartitionSpec as P


def column_weights(lower_order, first_column, columns_count, full_width):
    columns = first_column + jnp.arange(columns_count, dtype=jnp.int32)
    boundary = (full_width - 1 - lower_order)[:, None]
    lower_part = (columns[None, :] < boundary).astype(jnp.float32)
    upper_part = ((columns[None, :] >= boundary) & (columns[None, :] < full_width - 1)).astype(
        jnp.float32
    )
    lower_sign = (1 - 2 * (columns[None, :] % 2)).astype(jnp.float32)
    upper_sign = (1 - 2 * ((columns[None, :] + 1 + lower_order[:, None]) % 2)).astype(jnp.float32)
    return jnp.stack(
        [lower_part, lower_part * lower_sign, upper_part, upper_part * upper_sign], axis=1
    )


def spin_fields(plain, plus, minus):
    hemisphere = jnp.array([1.0, -1.0], jnp.float32).reshape(1, 1, 1, 2, 1, 1, 1)
    minus = minus * hemisphere
    temp_real = plain[:, :, :, :, 0]
    temp_imag = plain[:, :, :, :, 1]
    eplus_real = plus[:, :, :, :, 0, 0]
    eplus_imag = plus[:, :, :, :, 0, 1]
    bplus_real = plus[:, :, :, :, 1, 0]
    bplus_imag = plus[:, :, :, :, 1, 1]
    eminus_real = minus[:, :, :, :, 0, 0]
    eminus_imag = minus[:, :, :, :, 0, 1]
    bminus_real = minus[:, :, :, :, 1, 0]
    bminus_imag = minus[:, :, :, :, 1, 1]
    stokes_q_real = -(eplus_real - bminus_imag)
    stokes_q_imag = -(eplus_imag + bminus_real)
    stokes_u_real = -(bplus_real + eminus_imag)
    stokes_u_imag = -(bplus_imag - eminus_real)
    return jnp.stack(
        [
            jnp.stack([temp_real, temp_imag]),
            jnp.stack([stokes_q_real, stokes_q_imag]),
            jnp.stack([stokes_u_real, stokes_u_imag]),
        ]
    )


def place_orders(cycle_orders, lower_all):
    highest = lax.Precision.HIGHEST
    half = lower_all.shape[0]
    width = min(512, half)
    pieces = []
    for start in range(0, half, width):
        targets = start + jnp.arange(width, dtype=jnp.int32)
        onehot = (lower_all[:, None] == targets[None, :]).astype(jnp.float32)
        pieces.append(jnp.einsum("abcdes,sm->abcdem", cycle_orders, onehot, precision=highest))
    placed = jnp.concatenate(pieces, axis=-1)
    return jnp.concatenate([placed[..., 0, :], jnp.flip(placed[..., 1, :], axis=-1)], axis=-1)


def cycle_synthesis(coeff, shift, first_group, group_count):
    highest = lax.Precision.HIGHEST
    cycles_count = coeff.shape[0]
    components = coeff.shape[3]
    orders_count = coeff.shape[-1]
    pixels = 2 * orders_count
    outer = pixels // 128
    groups = orders_count // 128
    orders = jnp.arange(orders_count, dtype=jnp.int32)
    phase = (orders[None, :] * shift[:, None] % (2 * pixels)).astype(jnp.float32) * (
        math.pi / pixels
    )
    factor = jnp.where(orders == 0, 1.0, 2.0).astype(jnp.float32)
    cosine = (jnp.cos(phase) * factor)[:, None, None, :]
    sine = (jnp.sin(phase) * factor)[:, None, None, :]
    real_part = coeff[:, :, 0]
    imag_part = coeff[:, :, 1]
    shifted_real = (real_part * cosine - imag_part * sine).reshape(
        cycles_count, 3, components, groups, 128
    )
    shifted_imag = (real_part * sine + imag_part * cosine).reshape(
        cycles_count, 3, components, groups, 128
    )
    group_ids = jnp.arange(groups, dtype=jnp.int32)
    outer_ids = jnp.arange(outer, dtype=jnp.int32)
    inner_ids = jnp.arange(128, dtype=jnp.int32)
    angle_one = (group_ids[:, None] * outer_ids[None, :] % outer).astype(jnp.float32) * (
        2.0 * math.pi / outer
    )
    cos_one = jnp.cos(angle_one)
    sin_one = jnp.sin(angle_one)
    first_real = jnp.einsum(
        "xyzab,ak->xyzkb", shifted_real, cos_one, precision=highest
    ) - jnp.einsum("xyzab,ak->xyzkb", shifted_imag, sin_one, precision=highest)
    first_imag = jnp.einsum(
        "xyzab,ak->xyzkb", shifted_real, sin_one, precision=highest
    ) + jnp.einsum("xyzab,ak->xyzkb", shifted_imag, cos_one, precision=highest)
    angle_two = (outer_ids[:, None] * inner_ids[None, :] % pixels).astype(jnp.float32) * (
        2.0 * math.pi / pixels
    )
    cos_two = jnp.cos(angle_two)
    sin_two = jnp.sin(angle_two)
    twist_real = first_real * cos_two - first_imag * sin_two
    twist_imag = first_real * sin_two + first_imag * cos_two
    local_ids = first_group + jnp.arange(group_count, dtype=jnp.int32)
    angle_three = (inner_ids[:, None] * local_ids[None, :] % 128).astype(jnp.float32) * (
        2.0 * math.pi / 128
    )
    cos_three = jnp.cos(angle_three)
    sin_three = jnp.sin(angle_three)
    result = jnp.einsum("xyzkb,bq->xyzqk", twist_real, cos_three, precision=highest) - jnp.einsum(
        "xyzkb,bq->xyzqk", twist_imag, sin_three, precision=highest
    )
    return result.reshape(cycles_count, 3, components, group_count * outer)


def general_body(legendre, harmonics, slot_orders, cycle_index):
    ell_count = lax.axis_size("ell")
    slots_here = harmonics.shape[0]
    columns_here = harmonics.shape[-1]
    components = harmonics.shape[3]
    full_width = 2 * slot_orders.shape[0]
    pairs = cycle_index.shape[0]
    lower_here = lax.dynamic_slice_in_dim(
        slot_orders, lax.axis_index("ma") * slots_here, slots_here
    )
    weights = column_weights(
        lower_here, lax.axis_index("ell") * columns_here, columns_here, full_width
    ).astype(jnp.bfloat16)
    packed = harmonics[:, None] * weights[:, :, None, None, None, :]
    plain = jnp.einsum(
        "srj,sqpcj->srqpc", legendre[0], packed[:, :, 0], preferred_element_type=jnp.float32
    )
    plus = jnp.einsum(
        "srj,sqkpcj->srqkpc", legendre[1], packed[:, :, 1:3], preferred_element_type=jnp.float32
    )
    minus = jnp.einsum(
        "srj,sqkpcj->srqkpc", legendre[2], packed[:, :, 1:3], preferred_element_type=jnp.float32
    )
    plain = plain.reshape(slots_here, pairs, 2, 2, 2, components)
    plus = plus.reshape(slots_here, pairs, 2, 2, 2, 2, components)
    minus = minus.reshape(slots_here, pairs, 2, 2, 2, 2, components)
    fields = spin_fields(plain, plus, minus)
    cycle_sums = fields.transpose(5, 3, 0, 1, 6, 4, 2).reshape(
        2 * pairs, 3, 2, components, 2, slots_here
    )
    summed = lax.psum(cycle_sums, "ell")
    cycle_orders = lax.all_to_all(summed, "ma", split_axis=0, concat_axis=5, tiled=True)
    slot_ids = jnp.arange(slot_orders.shape[0], dtype=jnp.int32)
    lower_all = slot_orders[slot_ids]
    coeff = place_orders(cycle_orders, lower_all)
    cycles_here = cycle_orders.shape[0]
    cycle_ids = lax.axis_index("ma") * cycles_here + jnp.arange(cycles_here, dtype=jnp.int32)
    shift = cycle_index[cycle_ids % pairs] % 2
    per_device = 128 // ell_count
    return cycle_synthesis(coeff, shift, lax.axis_index("ell") * per_device, per_device)


LANES = 128
NT = (((1,), (1,)), ((), ()))


def rotate_sums(group, lane_tile, sub_pair):
    turned = None
    for step in range(4):
        mixed = group[step]
        for tile in range(1, 4):
            mixed = jnp.where(sub_pair == tile, group[(tile + step) % 4], mixed)
        if step == 0:
            turned = mixed
        else:
            mixed = pltpu.roll(mixed, 2 * step, 0)
            turned = jnp.where((sub_pair - lane_tile) % 4 == step, mixed, turned)
    return turned


def sums_kernel(full_width, columns, slots, orders_ref, table_ref, packed_ref, out_ref, part_ref):
    step = pl.program_id(0)
    block = table_ref.shape[1] // 8
    quads = block // 4
    first_slot = lax.axis_index("ma") * slots + step * block
    first_column = lax.axis_index("ell") * columns
    sub_pair = lax.broadcasted_iota(jnp.int32, (8, LANES), 0) // 2
    lane8 = lax.broadcasted_iota(jnp.int32, (8, LANES), 1)
    lane_tile = (lane8 % 16) // 4

    column = first_column + sub_pair * LANES + lane8
    alternate = (1 - 2 * (column % 2)).astype(jnp.float32)
    inside = column < full_width - 1

    def one_quad(quad, carry):
        base = pl.multiple_of(quad * 32, 32)
        parts = [[], [], [], []]
        for g in range(4):
            lower = orders_ref[first_slot + quad * 4 + g]
            is_lower = column < full_width - 1 - lower
            is_upper = jnp.logical_and(jnp.logical_not(is_lower), inside)
            upper_sign = alternate * (2 * (lower % 2) - 1).astype(jnp.float32)
            parts[0].append(jnp.where(is_lower, 1.0, 0.0))
            parts[1].append(jnp.where(is_lower, alternate, 0.0))
            parts[2].append(jnp.where(is_upper, 1.0, 0.0))
            parts[3].append(jnp.where(is_upper, upper_sign, 0.0))
        weights = [jnp.concatenate(p, axis=0).astype(jnp.bfloat16) for p in parts]
        tables = [table_ref[t, pl.ds(base, 32), :] for t in range(3)]
        first = pl.multiple_of(quad * 384, 32)
        where_to = pl.multiple_of((step * quads + quad) * 8, 8)
        left = jnp.concatenate([tables[0] * w for w in weights], axis=0)
        right = jnp.concatenate(
            [packed_ref[pl.ds(first + 96 * g, 32), :] for g in range(4)], axis=0
        )
        product = lax.dot_general(left, right, NT, preferred_element_type=jnp.float32)
        group = []
        for q in range(4):
            chosen = product[q * 32 : q * 32 + 8]
            for g in range(1, 4):
                chosen = jnp.where(
                    lane8 // 32 == g, product[q * 32 + g * 8 : q * 32 + g * 8 + 8], chosen
                )
            group.append(chosen)
        part_ref[0, pl.ds(where_to, 8), :] = rotate_sums(group, lane_tile, sub_pair)
        for p in range(2):
            left = jnp.concatenate(
                [
                    tables[t][p * 16 : p * 16 + 16] * w[p * 16 : p * 16 + 16]
                    for t in (1, 2)
                    for w in weights
                ],
                axis=0,
            )
            right = jnp.concatenate(
                [packed_ref[pl.ds(first + 96 * (2 * p + g) + 32, 64), :] for g in range(2)], axis=0
            )
            product = lax.dot_general(left, right, NT, preferred_element_type=jnp.float32)
            for t in range(2):
                group = []
                for q in range(4):
                    at = (t * 4 + q) * 16
                    group.append(
                        jnp.where(lane8 < 64, product[at : at + 8], product[at + 8 : at + 16])
                    )
                part_ref[1 + 2 * p + t, pl.ds(where_to, 8), :] = rotate_sums(
                    group, lane_tile, sub_pair
                )
        return carry

    lax.fori_loop(0, quads, one_quad, 0, unroll=UNROLL)

    @pl.when(step == pl.num_programs(0) - 1)
    def _():
        sub = lax.broadcasted_iota(jnp.int32, (8, LANES), 0)
        low = sub < 4
        turn_sign = jnp.where(low, -1.0, 1.0)

        def kind_tile(turned, at):
            real = turned[at : at + 8] + turned[at + 8 : at + 16]
            imag = turned[at + 16 : at + 24] + turned[at + 24 : at + 32]
            real = real + pltpu.roll(real, 4, 0)
            imag = imag + pltpu.roll(imag, 4, 0)
            return jnp.where(low, real, imag)

        for h in range(2):
            for south in range(2):
                for r in range(2):
                    qr = (h * 2 + south) * 2 + r
                    cycle = south * 2 + r
                    row0 = cycle * 24 * 8 + h * 4
                    turned = [
                        part_ref[i, pl.ds(qr, all_quads_static(part_ref), stride=8), :].T
                        for i in range(5)
                    ]
                    for g in range(4):
                        at = 64 * (g % 2)
                        plus = turned[1 + 2 * (g // 2)]
                        minus = turned[2 + 2 * (g // 2)]
                        temp = kind_tile(turned[0], g * 32)
                        e_plus = kind_tile(plus, at)
                        b_plus = kind_tile(plus, at + 32)
                        e_minus = kind_tile(minus, at)
                        b_minus = kind_tile(minus, at + 32)
                        hemisphere = turn_sign * (-1.0 if south else 1.0)
                        e_turn = pltpu.roll(e_minus, 4, 0) * hemisphere
                        b_turn = pltpu.roll(b_minus, 4, 0) * hemisphere
                        fields = (temp, -(e_plus + b_turn), e_turn - b_plus)
                        for f in range(3):
                            out_ref[pl.ds(row0 + f * 64 + g, 8, stride=8), :] = fields[f]


def all_quads_static(part_ref):
    return part_ref.shape[1] // 8


UNROLL = 2


def table_sums(legendre, harmonics, slot_orders):
    slots, columns = harmonics.shape[0], harmonics.shape[-1]
    full_width = 2 * slot_orders.shape[0]
    tables = (
        legendre.reshape(3, slots, 2, 4, LANES).transpose(0, 1, 3, 2, 4).reshape(3, slots * 8, LANES)
    )
    packed = (
        harmonics.reshape(slots, 3, 2, 4, 4, LANES)
        .transpose(0, 1, 2, 4, 3, 5)
        .reshape(slots * 96, LANES)
    )
    block = 32
    return pl.pallas_call(
        functools.partial(sums_kernel, full_width, columns, slots),
        grid=(slots // block,),
        in_specs=[
            pl.BlockSpec(memory_space=pltpu.SMEM),
            pl.BlockSpec((3, block * 8, LANES), lambda i: (0, i, 0)),
            pl.BlockSpec((block * 96, LANES), lambda i: (i, 0)),
        ],
        out_specs=pl.BlockSpec((768, LANES), lambda i: (0, 0)),
        out_shape=jax.ShapeDtypeStruct((768, LANES), jnp.float32),
        scratch_shapes=[
            pltpu.VMEM((5, slots * 2, LANES), jnp.float32),
        ],
        compiler_params=pltpu.CompilerParams(
            dimension_semantics=("arbitrary",), vmem_limit_bytes=64_000_000
        ),
    )(slot_orders, tables, packed)


def synthesis_kernel(
    scalars_ref, orders_ref, sums_ref, phase_ref, first_ref, twist_ref, last_ref, out_ref,
    left_ref, right_ref, held_ref, pixel_ref, landed_ref, send_sem, recv_sem, pixel_send, pixel_recv
):
    highest = lax.Precision.HIGHEST
    owners, sources = lax.axis_size("ma"), lax.axis_size("ell")
    my_owner, my_source = lax.axis_index("ma"), lax.axis_index("ell")
    me = my_owner * sources + my_source
    mesh_ids = pl.DeviceIdType.MESH
    count = owners * sources

    def shifted_device(step):
        owner = lax.rem(my_owner + step // sources, owners)
        source = lax.rem(my_source + step % sources, sources)
        return owner, source

    barrier = pltpu.get_barrier_semaphore()

    def greet(step, carry):
        pl.semaphore_signal(
            barrier, inc=1, device_id=shifted_device(step), device_id_type=mesh_ids
        )
        return carry

    lax.fori_loop(1, count, greet, 0)
    pl.semaphore_wait(barrier, count - 1)

    def exchange(step):
        owner, source = shifted_device(step)
        return pltpu.make_async_remote_copy(
            src_ref=sums_ref.at[owner * sources + source],
            dst_ref=held_ref.at[me],
            send_sem=send_sem.at[step],
            recv_sem=recv_sem.at[step],
            device_id=(owner, source),
            device_id_type=mesh_ids,
        )

    def send(step, carry):
        exchange(step).start()
        return carry

    lax.fori_loop(1, count, send, 0)
    held_ref[me] = sums_ref[me]

    tall = left_ref.shape[0] // 9
    tall_ids = lax.broadcasted_iota(jnp.int32, (tall, LANES), 0)
    lane_rows = lax.broadcasted_iota(jnp.int32, (LANES, LANES), 0)

    def await_step(step, carry):
        exchange(step).wait()
        return carry

    for near in range(owners):
        owner = lax.rem(my_owner + owners - near, owners)
        ordered = orders_ref[pl.ds(pl.multiple_of(owner * 8, 8), 8), :]
        for k in range(8):
            j = near * 8 + k
            right_ref[:, j * LANES : (j + 1) * LANES] = jnp.where(
                lane_rows == ordered[k : k + 1, :] % LANES, 1.0, 0.0
            ).astype(jnp.bfloat16)
    for near in range(owners):
        owner = lax.rem(my_owner + owners - near, owners)
        ordered = orders_ref[pl.ds(pl.multiple_of(owner * 8, 8), 8), :]
        lax.fori_loop(max(1, near * sources), (near + 1) * sources, await_step, 0)
        total = held_ref[owner * sources]
        for source in range(1, sources):
            total = total + held_ref[owner * sources + source]
        high = total.astype(jnp.bfloat16).astype(jnp.float32)
        rest = total - high
        middle = rest.astype(jnp.bfloat16).astype(jnp.float32)
        pieces = (high, middle, rest - middle)
        for k in range(8):
            j = near * 8 + k
            here = tall_ids == ordered[k : k + 1, :] // LANES
            for rr in range(3):
                for i in range(3):
                    at = (rr * 3 + i) * tall
                    piece = pieces[i][rr * 8 + k : rr * 8 + k + 1, :]
                    left_ref[at : at + tall, j * LANES : (j + 1) * LANES] = jnp.where(
                        here, piece, 0.0
                    ).astype(jnp.bfloat16)
    placed = lax.dot_general(
        left_ref[...], right_ref[...], NT, preferred_element_type=jnp.float32
    )
    shifted = scalars_ref[0] == 1
    factor = phase_ref[2]
    cosine = jnp.where(shifted, phase_ref[0], factor)
    sine = jnp.where(shifted, phase_ref[1], 0.0)
    half = 2 * tall

    def pixel_copy(rr, step):
        source = lax.rem(my_source + step, sources)
        rows = pl.ds(rr * 8, 8)
        return pltpu.make_async_remote_copy(
            src_ref=pixel_ref.at[source, rows],
            dst_ref=landed_ref.at[my_source, rows],
            send_sem=pixel_send.at[rr, step],
            recv_sem=pixel_recv.at[rr, step],
            device_id=(my_owner, source),
            device_id_type=mesh_ids,
        )

    for rr in range(3):
        at = rr * 3 * tall
        value = (
            placed[at : at + tall]
            + placed[at + tall : at + 2 * tall]
            + placed[at + 2 * tall : at + 3 * tall]
        )
        is_real = scalars_ref[1 + rr] == 0
        spectrum = jnp.concatenate(
            [
                value * jnp.where(is_real, cosine, -sine),
                value * jnp.where(is_real, sine, cosine),
            ],
            axis=0,
        )
        first = jnp.dot(
            first_ref[...], spectrum, precision=highest, preferred_element_type=jnp.float32
        )
        real, imag = first[:half], first[half:]
        twisted = jnp.concatenate(
            [
                real * twist_ref[0] - imag * twist_ref[1],
                real * twist_ref[1] + imag * twist_ref[0],
            ],
            axis=1,
        )
        both = lax.dot_general(
            last_ref[...], twisted, NT, precision=highest, preferred_element_type=jnp.float32
        )
        pixels = jnp.concatenate([both[:half], both[half:]], axis=1)
        for e in range(sources):
            pixel_ref[e, rr * 8 : rr * 8 + 8, :] = pixels[e * 8 : e * 8 + 8]
        if rr > 0:
            for step in range(1, sources):
                pixel_copy(rr - 1, step).start()
    landed_ref[my_source] = pixel_ref[my_source]
    for step in range(1, sources):
        pixel_copy(0, step).wait_send()
    for step in range(1, sources):
        pixel_copy(2, step).start()
    for step in range(1, sources):
        pixel_copy(0, step).wait_recv()
        pixel_copy(1, step).wait()
    for step in range(1, sources):
        pixel_copy(2, step).wait()
    for f in range(3):
        for c in range(4):
            real, imag = f * 8 + c, f * 8 + 4 + c
            out_ref[f * 4 + c] = (
                landed_ref[real // 3, real % 3 * 8 : real % 3 * 8 + 8]
                + landed_ref[imag // 3, imag % 3 * 8 : imag % 3 * 8 + 8]
            )


def synthesis_tables(orders_count):
    pixels = 2 * orders_count
    tall = orders_count // LANES
    half = 2 * tall
    orders = np.arange(orders_count).reshape(tall, LANES)
    factor = np.where(orders == 0, 1.0, 2.0)
    angle = orders * (np.pi / pixels)
    phase = np.stack([np.cos(angle) * factor, np.sin(angle) * factor, factor])
    angle = (np.arange(half)[:, None] * np.arange(tall)[None, :] % half) * (2 * np.pi / half)
    first = np.block([[np.cos(angle), -np.sin(angle)], [np.sin(angle), np.cos(angle)]])
    angle = np.arange(half)[:, None] * np.arange(LANES)[None, :] * (2 * np.pi / pixels)
    twist = np.stack([np.cos(angle), np.sin(angle)])
    ids = np.concatenate([np.arange(0, LANES, 2), np.arange(1, LANES, 2)])
    angle = (ids[:, None] * np.arange(LANES)[None, :] % LANES) * (2 * np.pi / LANES)
    last = np.concatenate([np.cos(angle), -np.sin(angle)], axis=1)
    return [jnp.asarray(t, jnp.float32) for t in (phase, first, twist, last)]


def synthesis(sums, orders, scalars, sources, orders_count):
    tall = orders_count // LANES
    vmem = pl.BlockSpec(memory_space=pltpu.VMEM)
    pixels = (sources, 24, LANES)
    return pl.pallas_call(
        synthesis_kernel,
        in_specs=[pl.BlockSpec(memory_space=pltpu.SMEM)] + [vmem] * 6,
        out_specs=vmem,
        out_shape=jax.ShapeDtypeStruct((12, 8, LANES), jnp.float32),
        scratch_shapes=[
            pltpu.VMEM((9 * tall, orders_count), jnp.bfloat16),
            pltpu.VMEM((LANES, orders_count), jnp.bfloat16),
            pltpu.VMEM(sums.shape, jnp.float32),
            pltpu.VMEM(pixels, jnp.float32),
            pltpu.VMEM(pixels, jnp.float32),
            pltpu.SemaphoreType.DMA((sums.shape[0],)),
            pltpu.SemaphoreType.DMA((sums.shape[0],)),
            pltpu.SemaphoreType.DMA((3, sources)),
            pltpu.SemaphoreType.DMA((3, sources)),
        ],
        compiler_params=pltpu.CompilerParams(
            vmem_limit_bytes=32 * 1024 * 1024, collective_id=0, has_side_effects=True
        ),
    )(scalars, orders, sums, *synthesis_tables(orders_count))


def slot_layout(slot_orders, owners):
    full_width = 2 * slot_orders.shape[0]
    lower = slot_orders.reshape(owners, LANES, 4).transpose(0, 2, 1)
    return jnp.stack([lower, full_width - 1 - lower], axis=1).reshape(owners * 8, LANES)


def packed_body(legendre, harmonics, slot_orders, cycle_index):
    owners = lax.axis_size("ma")
    sources = lax.axis_size("ell")
    full_width = 2 * slot_orders.shape[0]
    pairs = cycle_index.shape[0]
    me, part = lax.axis_index("ma"), lax.axis_index("ell")
    shift = cycle_index[me % pairs] % 2
    row = part * 3 + jnp.arange(3, dtype=jnp.int32)
    scalars = jnp.concatenate([shift[None], (row // 4) % 2])
    sums = table_sums(legendre, harmonics, slot_orders)
    maps = synthesis(
        sums.reshape(owners * sources, 24, LANES),
        slot_layout(slot_orders, owners),
        scalars,
        sources,
        full_width,
    )
    return maps.reshape(1, 3, 4, 8 * LANES)


def body(legendre, harmonics, slot_orders, cycle_index):
    owners, sources = lax.axis_size("ma"), lax.axis_size("ell")
    slots, kinds, parts, components, columns = harmonics.shape
    pairs = cycle_index.shape[0]
    fits = (
        (pairs, components, columns, slots) == (2, 4, 4 * LANES, 4 * LANES)
        and owners == 2 * pairs
        and kinds * parts * components == 3 * sources
        and slot_orders.shape[0] * 4 == sources * 8 * LANES
    )
    chosen = packed_body if fits else general_body
    return chosen(legendre, harmonics, slot_orders, cycle_index)


def solution(mesh):
    return jax.shard_map(
        body,
        mesh=mesh,
        in_specs=(P(None, "ma", None, "ell"), P("ma", None, None, None, "ell"), P(), P()),
        out_specs=P("ma", None, None, "ell"),
        check_vma=False,
    )
```

```python
import functools
import math

import jax
import jax.numpy as jnp
import numpy as np
from jax import lax
from jax.experimental import pallas as pl
from jax.experimental.pallas import tpu as pltpu
from jax.sharding import PartitionSpec as P


def column_weights(lower_order, first_column, columns_count, full_width):
    columns = first_column + jnp.arange(columns_count, dtype=jnp.int32)
    boundary = (full_width - 1 - lower_order)[:, None]
    lower_part = (columns[None, :] < boundary).astype(jnp.float32)
    upper_part = ((columns[None, :] >= boundary) & (columns[None, :] < full_width - 1)).astype(
        jnp.float32
    )
    lower_sign = (1 - 2 * (columns[None, :] % 2)).astype(jnp.float32)
    upper_sign = (1 - 2 * ((columns[None, :] + 1 + lower_order[:, None]) % 2)).astype(jnp.float32)
    return jnp.stack(
        [lower_part, lower_part * lower_sign, upper_part, upper_part * upper_sign], axis=1
    )


def spin_fields(plain, plus, minus):
    hemisphere = jnp.array([1.0, -1.0], jnp.float32).reshape(1, 1, 1, 2, 1, 1, 1)
    minus = minus * hemisphere
    temp_real = plain[:, :, :, :, 0]
    temp_imag = plain[:, :, :, :, 1]
    eplus_real = plus[:, :, :, :, 0, 0]
    eplus_imag = plus[:, :, :, :, 0, 1]
    bplus_real = plus[:, :, :, :, 1, 0]
    bplus_imag = plus[:, :, :, :, 1, 1]
    eminus_real = minus[:, :, :, :, 0, 0]
    eminus_imag = minus[:, :, :, :, 0, 1]
    bminus_real = minus[:, :, :, :, 1, 0]
    bminus_imag = minus[:, :, :, :, 1, 1]
    stokes_q_real = -(eplus_real - bminus_imag)
    stokes_q_imag = -(eplus_imag + bminus_real)
    stokes_u_real = -(bplus_real + eminus_imag)
    stokes_u_imag = -(bplus_imag - eminus_real)
    return jnp.stack(
        [
            jnp.stack([temp_real, temp_imag]),
            jnp.stack([stokes_q_real, stokes_q_imag]),
            jnp.stack([stokes_u_real, stokes_u_imag]),
        ]
    )


def place_orders(cycle_orders, lower_all):
    highest = lax.Precision.HIGHEST
    half = lower_all.shape[0]
    width = min(512, half)
    pieces = []
    for start in range(0, half, width):
        targets = start + jnp.arange(width, dtype=jnp.int32)
        onehot = (lower_all[:, None] == targets[None, :]).astype(jnp.float32)
        pieces.append(jnp.einsum("abcdes,sm->abcdem", cycle_orders, onehot, precision=highest))
    placed = jnp.concatenate(pieces, axis=-1)
    return jnp.concatenate([placed[..., 0, :], jnp.flip(placed[..., 1, :], axis=-1)], axis=-1)


def cycle_synthesis(coeff, shift, first_group, group_count):
    highest = lax.Precision.HIGHEST
    cycles_count = coeff.shape[0]
    components = coeff.shape[3]
    orders_count = coeff.shape[-1]
    pixels = 2 * orders_count
    outer = pixels // 128
    groups = orders_count // 128
    orders = jnp.arange(orders_count, dtype=jnp.int32)
    phase = (orders[None, :] * shift[:, None] % (2 * pixels)).astype(jnp.float32) * (
        math.pi / pixels
    )
    factor = jnp.where(orders == 0, 1.0, 2.0).astype(jnp.float32)
    cosine = (jnp.cos(phase) * factor)[:, None, None, :]
    sine = (jnp.sin(phase) * factor)[:, None, None, :]
    real_part = coeff[:, :, 0]
    imag_part = coeff[:, :, 1]
    shifted_real = (real_part * cosine - imag_part * sine).reshape(
        cycles_count, 3, components, groups, 128
    )
    shifted_imag = (real_part * sine + imag_part * cosine).reshape(
        cycles_count, 3, components, groups, 128
    )
    group_ids = jnp.arange(groups, dtype=jnp.int32)
    outer_ids = jnp.arange(outer, dtype=jnp.int32)
    inner_ids = jnp.arange(128, dtype=jnp.int32)
    angle_one = (group_ids[:, None] * outer_ids[None, :] % outer).astype(jnp.float32) * (
        2.0 * math.pi / outer
    )
    cos_one = jnp.cos(angle_one)
    sin_one = jnp.sin(angle_one)
    first_real = jnp.einsum(
        "xyzab,ak->xyzkb", shifted_real, cos_one, precision=highest
    ) - jnp.einsum("xyzab,ak->xyzkb", shifted_imag, sin_one, precision=highest)
    first_imag = jnp.einsum(
        "xyzab,ak->xyzkb", shifted_real, sin_one, precision=highest
    ) + jnp.einsum("xyzab,ak->xyzkb", shifted_imag, cos_one, precision=highest)
    angle_two = (outer_ids[:, None] * inner_ids[None, :] % pixels).astype(jnp.float32) * (
        2.0 * math.pi / pixels
    )
    cos_two = jnp.cos(angle_two)
    sin_two = jnp.sin(angle_two)
    twist_real = first_real * cos_two - first_imag * sin_two
    twist_imag = first_real * sin_two + first_imag * cos_two
    local_ids = first_group + jnp.arange(group_count, dtype=jnp.int32)
    angle_three = (inner_ids[:, None] * local_ids[None, :] % 128).astype(jnp.float32) * (
        2.0 * math.pi / 128
    )
    cos_three = jnp.cos(angle_three)
    sin_three = jnp.sin(angle_three)
    result = jnp.einsum("xyzkb,bq->xyzqk", twist_real, cos_three, precision=highest) - jnp.einsum(
        "xyzkb,bq->xyzqk", twist_imag, sin_three, precision=highest
    )
    return result.reshape(cycles_count, 3, components, group_count * outer)


def general_body(legendre, harmonics, slot_orders, cycle_index):
    ell_count = lax.axis_size("ell")
    slots_here = harmonics.shape[0]
    columns_here = harmonics.shape[-1]
    components = harmonics.shape[3]
    full_width = 2 * slot_orders.shape[0]
    pairs = cycle_index.shape[0]
    lower_here = lax.dynamic_slice_in_dim(
        slot_orders, lax.axis_index("ma") * slots_here, slots_here
    )
    weights = column_weights(
        lower_here, lax.axis_index("ell") * columns_here, columns_here, full_width
    ).astype(jnp.bfloat16)
    packed = harmonics[:, None] * weights[:, :, None, None, None, :]
    plain = jnp.einsum(
        "srj,sqpcj->srqpc", legendre[0], packed[:, :, 0], preferred_element_type=jnp.float32
    )
    plus = jnp.einsum(
        "srj,sqkpcj->srqkpc", legendre[1], packed[:, :, 1:3], preferred_element_type=jnp.float32
    )
    minus = jnp.einsum(
        "srj,sqkpcj->srqkpc", legendre[2], packed[:, :, 1:3], preferred_element_type=jnp.float32
    )
    plain = plain.reshape(slots_here, pairs, 2, 2, 2, components)
    plus = plus.reshape(slots_here, pairs, 2, 2, 2, 2, components)
    minus = minus.reshape(slots_here, pairs, 2, 2, 2, 2, components)
    fields = spin_fields(plain, plus, minus)
    cycle_sums = fields.transpose(5, 3, 0, 1, 6, 4, 2).reshape(
        2 * pairs, 3, 2, components, 2, slots_here
    )
    summed = lax.psum(cycle_sums, "ell")
    cycle_orders = lax.all_to_all(summed, "ma", split_axis=0, concat_axis=5, tiled=True)
    slot_ids = jnp.arange(slot_orders.shape[0], dtype=jnp.int32)
    lower_all = slot_orders[slot_ids]
    coeff = place_orders(cycle_orders, lower_all)
    cycles_here = cycle_orders.shape[0]
    cycle_ids = lax.axis_index("ma") * cycles_here + jnp.arange(cycles_here, dtype=jnp.int32)
    shift = cycle_index[cycle_ids % pairs] % 2
    per_device = 128 // ell_count
    return cycle_synthesis(coeff, shift, lax.axis_index("ell") * per_device, per_device)


LANES = 128
NT = (((1,), (1,)), ((), ()))


def rotate_sums(group, lane_tile, sub_pair):
    turned = None
    for step in range(4):
        mixed = group[step]
        for tile in range(1, 4):
            mixed = jnp.where(sub_pair == tile, group[(tile + step) % 4], mixed)
        if step == 0:
            turned = mixed
        else:
            mixed = pltpu.roll(mixed, 2 * step, 0)
            turned = jnp.where((sub_pair - lane_tile) % 4 == step, mixed, turned)
    return turned


def sums_kernel(full_width, columns, slots, orders_ref, table_ref, packed_ref, out_ref, part_ref):
    step = pl.program_id(0)
    quads = table_ref.shape[2] // 8
    stride = slots // 4
    first_slot = lax.axis_index("ma") * slots + step * quads
    first_column = lax.axis_index("ell") * columns
    sub_pair = lax.broadcasted_iota(jnp.int32, (8, LANES), 0) // 2
    lane8 = lax.broadcasted_iota(jnp.int32, (8, LANES), 1)
    lane_tile = (lane8 % 16) // 4

    column = first_column + sub_pair * LANES + lane8
    alternate = (1 - 2 * (column % 2)).astype(jnp.float32)
    inside = column < full_width - 1

    def one_quad(quad, carry):
        eight = pl.ds(pl.multiple_of(quad * 8, 8), 8)
        weights = []
        for g in range(4):
            lower = orders_ref[first_slot + g * stride + quad]
            is_lower = column < full_width - 1 - lower
            is_upper = jnp.logical_and(jnp.logical_not(is_lower), inside)
            upper_sign = alternate * (2 * (lower % 2) - 1).astype(jnp.float32)
            weights.append(
                (
                    jnp.where(is_lower, 1.0, 0.0),
                    jnp.where(is_lower, alternate, 0.0),
                    jnp.where(is_upper, 1.0, 0.0),
                    jnp.where(is_upper, upper_sign, 0.0),
                )
            )

        def weighted(kinds, members):
            values = {
                (t, g): table_ref[t, g, eight, :].astype(jnp.float32)
                for t in kinds
                for g in members
            }
            return jnp.concatenate(
                [values[t, g] * weights[g][q] for t in kinds for q in range(4) for g in members],
                axis=0,
            ).astype(jnp.bfloat16)

        first = pl.multiple_of(quad * 96, 32)
        where_to = pl.multiple_of((step * quads + quad) * 8, 8)
        left = weighted((0,), range(4))
        right = jnp.concatenate(
            [packed_ref[g, pl.ds(first, 32), :] for g in range(4)], axis=0
        )
        product = lax.dot_general(left, right, NT, preferred_element_type=jnp.float32)
        group = []
        for q in range(4):
            chosen = product[q * 32 : q * 32 + 8]
            for g in range(1, 4):
                chosen = jnp.where(
                    lane8 // 32 == g, product[q * 32 + g * 8 : q * 32 + g * 8 + 8], chosen
                )
            group.append(chosen)
        part_ref[0, pl.ds(where_to, 8), :] = rotate_sums(group, lane_tile, sub_pair)
        for p in range(2):
            left = weighted((1, 2), (2 * p, 2 * p + 1))
            right = jnp.concatenate(
                [packed_ref[2 * p + g, pl.ds(first + 32, 64), :] for g in range(2)], axis=0
            )
            product = lax.dot_general(left, right, NT, preferred_element_type=jnp.float32)
            for t in range(2):
                group = []
                for q in range(4):
                    at = (t * 4 + q) * 16
                    group.append(
                        jnp.where(lane8 < 64, product[at : at + 8], product[at + 8 : at + 16])
                    )
                part_ref[1 + 2 * p + t, pl.ds(where_to, 8), :] = rotate_sums(
                    group, lane_tile, sub_pair
                )
        return carry

    lax.fori_loop(0, quads, one_quad, 0, unroll=UNROLL)

    @pl.when(step == pl.num_programs(0) - 1)
    def _():
        sub = lax.broadcasted_iota(jnp.int32, (8, LANES), 0)
        low = sub < 4
        turn_sign = jnp.where(low, -1.0, 1.0)

        def kind_tile(turned, at):
            real = turned[at : at + 8] + turned[at + 8 : at + 16]
            imag = turned[at + 16 : at + 24] + turned[at + 24 : at + 32]
            real = real + pltpu.roll(real, 4, 0)
            imag = imag + pltpu.roll(imag, 4, 0)
            return jnp.where(low, real, imag)

        for h in range(2):
            for south in range(2):
                for r in range(2):
                    qr = (h * 2 + south) * 2 + r
                    cycle = south * 2 + r
                    row0 = cycle * 24 * 8 + h * 4
                    turned = [
                        part_ref[i, pl.ds(qr, all_quads_static(part_ref), stride=8), :].T
                        for i in range(5)
                    ]
                    for g in range(4):
                        at = 64 * (g % 2)
                        plus = turned[1 + 2 * (g // 2)]
                        minus = turned[2 + 2 * (g // 2)]
                        temp = kind_tile(turned[0], g * 32)
                        e_plus = kind_tile(plus, at)
                        b_plus = kind_tile(plus, at + 32)
                        e_minus = kind_tile(minus, at)
                        b_minus = kind_tile(minus, at + 32)
                        hemisphere = turn_sign * (-1.0 if south else 1.0)
                        e_turn = pltpu.roll(e_minus, 4, 0) * hemisphere
                        b_turn = pltpu.roll(b_minus, 4, 0) * hemisphere
                        fields = (temp, -(e_plus + b_turn), e_turn - b_plus)
                        for f in range(3):
                            out_ref[pl.ds(row0 + f * 64 + g, 8, stride=8), :] = fields[f]


def all_quads_static(part_ref):
    return part_ref.shape[1] // 8


UNROLL = 16
BLOCK = 64


def table_sums(legendre, harmonics, slot_orders):
    slots, columns = harmonics.shape[0], harmonics.shape[-1]
    full_width = 2 * slot_orders.shape[0]
    tables = (
        legendre.reshape(3, slots, 2, 4, LANES).transpose(0, 1, 3, 2, 4).reshape(3, 4, slots * 2, LANES)
    )
    packed = (
        harmonics.reshape(slots, 3, 2, 4, 4, LANES)
        .transpose(0, 1, 2, 4, 3, 5)
        .reshape(4, slots * 24, LANES)
    )
    block = BLOCK
    return pl.pallas_call(
        functools.partial(sums_kernel, full_width, columns, slots),
        grid=(slots // block,),
        in_specs=[
            pl.BlockSpec(memory_space=pltpu.SMEM),
            pl.BlockSpec((3, 4, block * 2, LANES), lambda i: (0, 0, i, 0)),
            pl.BlockSpec((4, block * 24, LANES), lambda i: (0, i, 0)),
        ],
        out_specs=pl.BlockSpec((768, LANES), lambda i: (0, 0)),
        out_shape=jax.ShapeDtypeStruct((768, LANES), jnp.float32),
        scratch_shapes=[
            pltpu.VMEM((5, slots * 2, LANES), jnp.float32),
        ],
        compiler_params=pltpu.CompilerParams(
            dimension_semantics=("arbitrary",), vmem_limit_bytes=64_000_000
        ),
    )(slot_orders, tables, packed)


def synthesis_kernel(
    width, cycle_ref, orders_ref, sums_ref, phase_ref, first_ref, twist_ref, last_ref, out_ref,
    left_ref, right_ref, held_ref, pixel_ref, landed_ref, send_sem, recv_sem, pixel_send, pixel_recv
):
    highest = lax.Precision.HIGHEST
    owners, sources = lax.axis_size("ma"), lax.axis_size("ell")
    my_owner, my_source = lax.axis_index("ma"), lax.axis_index("ell")
    me = my_owner * sources + my_source
    mesh_ids = pl.DeviceIdType.MESH
    count = owners * sources

    def shifted_device(step):
        owner = lax.rem(my_owner + step // sources, owners)
        source = lax.rem(my_source + step % sources, sources)
        return owner, source

    barrier = pltpu.get_barrier_semaphore()

    def greet(step, carry):
        pl.semaphore_signal(
            barrier, inc=1, device_id=shifted_device(step), device_id_type=mesh_ids
        )
        return carry

    lax.fori_loop(1, count, greet, 0)
    pl.semaphore_wait(barrier, count - 1)

    def exchange(step):
        owner, source = shifted_device(step)
        return pltpu.make_async_remote_copy(
            src_ref=sums_ref.at[owner * sources + source],
            dst_ref=held_ref.at[me],
            send_sem=send_sem.at[step],
            recv_sem=recv_sem.at[step],
            device_id=(owner, source),
            device_id_type=mesh_ids,
        )

    def send(step, carry):
        exchange(step).start()
        return carry

    lax.fori_loop(1, count, send, 0)
    held_ref[me] = sums_ref[me]

    tall = left_ref.shape[0] // 9
    tall_ids = lax.broadcasted_iota(jnp.int32, (tall, LANES), 0)
    lane_rows = lax.broadcasted_iota(jnp.int32, (LANES, LANES), 0)

    def order_rows(owner):
        lower = orders_ref[owner]
        return jnp.concatenate([lower, width - 1 - lower], axis=0)

    def await_step(step, carry):
        exchange(step).wait()
        return carry

    for near in range(owners):
        owner = lax.rem(my_owner + owners - near, owners)
        ordered = order_rows(owner)
        for k in range(8):
            j = near * 8 + k
            right_ref[:, j * LANES : (j + 1) * LANES] = jnp.where(
                lane_rows == ordered[k : k + 1, :] % LANES, 1.0, 0.0
            ).astype(jnp.bfloat16)
    for near in range(owners):
        owner = lax.rem(my_owner + owners - near, owners)
        ordered = order_rows(owner)
        lax.fori_loop(max(1, near * sources), (near + 1) * sources, await_step, 0)
        total = held_ref[owner * sources]
        for source in range(1, sources):
            total = total + held_ref[owner * sources + source]
        high = total.astype(jnp.bfloat16).astype(jnp.float32)
        rest = total - high
        middle = rest.astype(jnp.bfloat16).astype(jnp.float32)
        pieces = (high, middle, rest - middle)
        for k in range(8):
            j = near * 8 + k
            here = tall_ids == ordered[k : k + 1, :] // LANES
            for rr in range(3):
                for i in range(3):
                    at = (rr * 3 + i) * tall
                    piece = pieces[i][rr * 8 + k : rr * 8 + k + 1, :]
                    left_ref[at : at + tall, j * LANES : (j + 1) * LANES] = jnp.where(
                        here, piece, 0.0
                    ).astype(jnp.bfloat16)
    placed = lax.dot_general(
        left_ref[...], right_ref[...], NT, preferred_element_type=jnp.float32
    )
    shifted = cycle_ref[lax.rem(my_owner, cycle_ref.shape[0])] % 2 == 1
    factor = phase_ref[2]
    cosine = jnp.where(shifted, phase_ref[0], factor)
    sine = jnp.where(shifted, phase_ref[1], 0.0)
    half = 2 * tall

    def pixel_copy(rr, step):
        source = lax.rem(my_source + step, sources)
        rows = pl.ds(rr * 8, 8)
        return pltpu.make_async_remote_copy(
            src_ref=pixel_ref.at[source, rows],
            dst_ref=landed_ref.at[my_source, rows],
            send_sem=pixel_send.at[rr, step],
            recv_sem=pixel_recv.at[rr, step],
            device_id=(my_owner, source),
            device_id_type=mesh_ids,
        )

    for rr in range(3):
        at = rr * 3 * tall
        value = (
            placed[at : at + tall]
            + placed[at + tall : at + 2 * tall]
            + placed[at + 2 * tall : at + 3 * tall]
        )
        is_real = (my_source * 3 + rr) // 4 % 2 == 0
        spectrum = jnp.concatenate(
            [
                value * jnp.where(is_real, cosine, -sine),
                value * jnp.where(is_real, sine, cosine),
            ],
            axis=0,
        )
        first = jnp.dot(
            first_ref[...], spectrum, precision=highest, preferred_element_type=jnp.float32
        )
        real, imag = first[:half], first[half:]
        twisted = jnp.concatenate(
            [
                real * twist_ref[0] - imag * twist_ref[1],
                real * twist_ref[1] + imag * twist_ref[0],
            ],
            axis=1,
        )
        both = lax.dot_general(
            last_ref[...], twisted, NT, precision=highest, preferred_element_type=jnp.float32
        )
        pixels = jnp.concatenate([both[:half], both[half:]], axis=1)
        for e in range(sources):
            pixel_ref[e, rr * 8 : rr * 8 + 8, :] = pixels[e * 8 : e * 8 + 8]
        if rr > 0:
            for step in range(1, sources):
                pixel_copy(rr - 1, step).start()
    landed_ref[my_source] = pixel_ref[my_source]
    for step in range(1, sources):
        pixel_copy(0, step).wait_send()
    for step in range(1, sources):
        pixel_copy(2, step).start()
    for step in range(1, sources):
        pixel_copy(0, step).wait_recv()
        pixel_copy(1, step).wait()
    for step in range(1, sources):
        pixel_copy(2, step).wait()
    for f in range(3):
        for c in range(4):
            real, imag = f * 8 + c, f * 8 + 4 + c
            out_ref[f * 4 + c] = (
                landed_ref[real // 3, real % 3 * 8 : real % 3 * 8 + 8]
                + landed_ref[imag // 3, imag % 3 * 8 : imag % 3 * 8 + 8]
            )


def synthesis_tables(orders_count):
    pixels = 2 * orders_count
    tall = orders_count // LANES
    half = 2 * tall
    orders = np.arange(orders_count).reshape(tall, LANES)
    factor = np.where(orders == 0, 1.0, 2.0)
    angle = orders * (np.pi / pixels)
    phase = np.stack([np.cos(angle) * factor, np.sin(angle) * factor, factor])
    angle = (np.arange(half)[:, None] * np.arange(tall)[None, :] % half) * (2 * np.pi / half)
    first = np.block([[np.cos(angle), -np.sin(angle)], [np.sin(angle), np.cos(angle)]])
    angle = np.arange(half)[:, None] * np.arange(LANES)[None, :] * (2 * np.pi / pixels)
    twist = np.stack([np.cos(angle), np.sin(angle)])
    ids = np.concatenate([np.arange(0, LANES, 2), np.arange(1, LANES, 2)])
    angle = (ids[:, None] * np.arange(LANES)[None, :] % LANES) * (2 * np.pi / LANES)
    last = np.concatenate([np.cos(angle), -np.sin(angle)], axis=1)
    return [jnp.asarray(t, jnp.float32) for t in (phase, first, twist, last)]


def synthesis(sums, slot_orders, cycle_index, owners, sources):
    orders_count = 2 * slot_orders.shape[0]
    tall = orders_count // LANES
    vmem = pl.BlockSpec(memory_space=pltpu.VMEM)
    pixels = (sources, 24, LANES)
    return pl.pallas_call(
        functools.partial(synthesis_kernel, orders_count),
        in_specs=[pl.BlockSpec(memory_space=pltpu.SMEM)] + [vmem] * 6,
        out_specs=vmem,
        out_shape=jax.ShapeDtypeStruct((12, 8, LANES), jnp.float32),
        scratch_shapes=[
            pltpu.VMEM((9 * tall, orders_count), jnp.bfloat16),
            pltpu.VMEM((LANES, orders_count), jnp.bfloat16),
            pltpu.VMEM(sums.shape, jnp.float32),
            pltpu.VMEM(pixels, jnp.float32),
            pltpu.VMEM(pixels, jnp.float32),
            pltpu.SemaphoreType.DMA((sums.shape[0],)),
            pltpu.SemaphoreType.DMA((sums.shape[0],)),
            pltpu.SemaphoreType.DMA((3, sources)),
            pltpu.SemaphoreType.DMA((3, sources)),
        ],
        compiler_params=pltpu.CompilerParams(
            vmem_limit_bytes=32 * 1024 * 1024, collective_id=0, has_side_effects=True
        ),
    )(cycle_index, slot_orders.reshape(owners, 4, LANES), sums, *synthesis_tables(orders_count))


def packed_body(legendre, harmonics, slot_orders, cycle_index):
    owners = lax.axis_size("ma")
    sources = lax.axis_size("ell")
    sums = table_sums(legendre, harmonics, slot_orders)
    maps = synthesis(
        sums.reshape(owners * sources, 24, LANES), slot_orders, cycle_index, owners, sources
    )
    return maps.reshape(1, 3, 4, 8 * LANES)


def body(legendre, harmonics, slot_orders, cycle_index):
    owners, sources = lax.axis_size("ma"), lax.axis_size("ell")
    slots, kinds, parts, components, columns = harmonics.shape
    pairs = cycle_index.shape[0]
    fits = (
        (pairs, components, columns, slots) == (2, 4, 4 * LANES, 4 * LANES)
        and owners == 2 * pairs
        and kinds * parts * components == 3 * sources
        and slot_orders.shape[0] * 4 == sources * 8 * LANES
    )
    chosen = packed_body if fits else general_body
    return chosen(legendre, harmonics, slot_orders, cycle_index)


def solution(mesh):
    return jax.shard_map(
        body,
        mesh=mesh,
        in_specs=(P(None, "ma", None, "ell"), P("ma", None, None, None, "ell"), P(), P()),
        out_specs=P("ma", None, None, "ell"),
        check_vma=False,
    )
```
